32 devices in a mesh: prow: 4 (over y, core), pcol: 8 (over z, x).
Axes of the slice: x: 2, y: 2, z: 4, core: 2. Of those that a mesh axis runs over, the one named last changes fastest.
Arguments:
- slab: bfloat16 [8192, 3072], P('prow', 'pcol'), may hold values from -6 to 6
- pivots: int32 [512], replicated, may hold values from 0 to 8191, as said below
- l_top: bfloat16 [512, 512], replicated, may hold values from -0.125 to 0.125
- l_panel_t: bfloat16 [512, 8192], P('pcol', 'prow'), may hold values from -0.125 to 0.125
Outputs:
- result: bfloat16 [8192, 3072], P('prow', 'pcol')
The draws below stay inside these ranges and needn't reach their ends.
Inputs may be any that keep to these rules, and one draw needn't show every extreme that they name: `pivots`: distinct rows; how many fall on each index of prow is uneven and changes with the draw.
All inputs are finite; a program needn't handle non-finite values.
Results may differ from the reference program's by a relative error of at most 0.0029.
Values may be sent and summed in bfloat16 or wider, within the bound.
A program may use at most 64 MiB of HBM per device.

```python
import jax
import jax.numpy as jnp
from jax import lax

NB = 512
ROW_DEV = 2048
ROWS = 8192
COLS = 3072
N_PROW = 4


def draw_pivots(key, part):
    first_key, second_key, third_key = jax.random.split(key, 3)
    weights = jax.random.randint(first_key, (N_PROW,), 1, 9)
    cumulative = jnp.cumsum(weights)
    picks = jax.random.randint(second_key, (NB,), 0, cumulative[-1])
    owner = jnp.sum((picks[:, None] >= cumulative[None, :]).astype(jnp.int32), axis=1)
    onehot = (owner[:, None] == jnp.arange(N_PROW, dtype=jnp.int32)[None, :]).astype(jnp.int32)
    ranks = jnp.sum((jnp.cumsum(onehot, axis=0) - onehot) * onehot, axis=1)
    owner_keys = jax.random.split(third_key, N_PROW)
    orders = jax.vmap(lambda k: jax.random.permutation(k, ROW_DEV))(owner_keys)
    local = orders[owner, ranks]
    return (owner * ROW_DEV + local).astype(jnp.int32)


def shard_levels(rng, extent, pieces, low, high):
    def one(position, shards_of):
        heights = jax.random.uniform(jax.random.fold_in(jax.random.fold_in(rng, 6), position), (shards_of,), jnp.float32, low / len(pieces), high / len(pieces))
        return jnp.repeat(jnp.exp(heights), extent[position] // shards_of).reshape((-1,) + (1,) * (len(extent) - position - 1))

    level = one(*pieces[0])
    for cut in pieces[1:]:
        level = level * one(*cut)
    return level


def centred(stream_key, dims, deviation, reach, shards=(), kind=jnp.bfloat16):
    entries = jax.random.normal(stream_key, dims, jnp.float32) * deviation
    if len(shards) > 0:
        entries = shard_levels(stream_key, dims, shards, -0.22, 0.18) * entries
    return jnp.clip(entries, min=-reach, max=reach).astype(kind)


def setup_inputs(seed: int = 0) -> dict:
    streams_of = jax.random.split(jax.random.key(seed), 5)
    return {
        "slab": centred(streams_of[0], (ROWS, COLS), 1.0, 6.0, ((0, 4), (1, 8))),
        "pivots": draw_pivots(jax.random.fold_in(streams_of[4], 71), 0),
        "l_top": centred(streams_of[2], (NB, NB), (4 * NB) ** -0.5, 0.125),
        "l_panel_t": centred(streams_of[3], (NB, ROWS), (4 * NB) ** -0.5, 0.125, ((0, 8), (1, 4))),
    }


def bookkeeping(pivots):
    index = jnp.arange(NB, dtype=jnp.int32)
    chosen = jnp.any(pivots[:, None] == index[None, :], axis=0)
    free = jnp.logical_not(chosen)
    free_rank = jnp.cumsum(free.astype(jnp.int32)) - 1
    far = pivots >= NB
    far_rank = jnp.cumsum(far.astype(jnp.int32)) - 1
    match = free[None, :] & (free_rank[None, :] == far_rank[:, None])
    source = jnp.sum(jnp.where(match, index[None, :], 0), axis=1).astype(jnp.int32)
    return (far, source)

def reference(slab, pivots, l_top, l_panel_t):
    total_rows = slab.shape[0]
    far, source = bookkeeping(pivots)
    target = jnp.where(far, pivots, total_rows).astype(jnp.int32)
    pivoted = slab.at[target].set(slab[source], mode='drop')
    top = slab[pivots]
    lower = jnp.tril(l_top.astype(jnp.float32), -1) + jnp.eye(NB, dtype=jnp.float32)
    upper = lax.linalg.triangular_solve(lower, top.astype(jnp.float32), left_side=True, lower=True, unit_diagonal=True)
    u_block = upper.astype(jnp.bfloat16)
    u_wide = u_block.astype(jnp.float32)
    blocks = pivoted.reshape(N_PROW, ROW_DEV, -1)
    panels = jnp.transpose(l_panel_t.reshape(NB, N_PROW, ROW_DEV), (1, 0, 2))

    def one_block(pair):
        rows_here, panel_here = pair
        product = jnp.dot(panel_here.astype(jnp.float32).T.astype(jnp.float32), u_wide.astype(jnp.float32), preferred_element_type=jnp.float32)
        return (rows_here.astype(jnp.float32) - product).astype(jnp.bfloat16)
    updated = lax.map(one_block, (blocks, panels)).reshape(total_rows, -1)
    return updated.at[:NB].set(u_block)
```

```python
import functools

import jax
import jax.numpy as jnp
from jax import lax
from jax.experimental import pallas as pl
from jax.experimental.pallas import tpu as pltpu
from jax.sharding import PartitionSpec as P

MESH = pl.DeviceIdType.MESH
F32 = jnp.float32
BF16 = jnp.bfloat16
LANES = 128


def dot(a, b):
    return jnp.dot(a, b, preferred_element_type=F32)


def dot_high(a, b):
    return jnp.dot(a, b, preferred_element_type=F32, precision=lax.Precision.HIGHEST)


def iota(shape, axis):
    return lax.broadcasted_iota(jnp.int32, shape, axis)


def cuts(width):
    units = width // LANES
    first = (units * 7) // 16
    second = (units * 13) // 16
    edges = (0, first * LANES, second * LANES, width)
    return [(a, b - a) for a, b in zip(edges[:-1], edges[1:])]


def kernel(
    n_prow, n_pcol,
    slab_hbm, pivots_ref, l_top_ref, panel_hbm, out_ref,
    slab_ref, gathered, picked, picked_in, merged, homes, pivoted, inverse_hi, inverse_lo, high, u_ref,
    local_sem, panel_recv, panel_send, core_sem, chip_send, chip_recv, relay_send, relay_recv,
):
    block = l_top_ref.shape[0]
    rows, width = slab_ref.shape
    me_r = lax.axis_index("prow")
    me_c = lax.axis_index("pcol")
    chips = n_prow // 2
    chip, core = me_r // 2, me_r % 2
    peer = me_r + 1 - 2 * core
    length = n_pcol // 2
    z, x = me_c // 2, me_c % 2
    other = 1 - x
    pieces = cuts(gathered.shape[2])
    bulk = range(len(pieces) - 1)
    rest = len(pieces) - 1

    slab_copy = pltpu.make_async_copy(slab_hbm, slab_ref, local_sem.at[0])
    panel_copy = pltpu.make_async_copy(panel_hbm, gathered.at[me_c], local_sem.at[1])
    panel_copy.start()
    slab_copy.start()

    barrier = pltpu.get_barrier_semaphore()

    def greet(r, c):
        pl.semaphore_signal(barrier, inc=1, device_id=(r, c), device_id_type=MESH)

    greet(peer, me_c)
    greet(me_r, z * 2 + other)
    for step in range(1, chips):
        greet(((chip + step) % chips) * 2 + core, me_c)

    @pl.when(z > 0)
    def _():
        greet(me_r, me_c - 2)

    @pl.when(z < length - 1)
    def _():
        greet(me_r, me_c + 2)

    has_below = (z + length - 1) // length
    has_above = (2 * length - 2 - z) // length
    pl.semaphore_wait(barrier, 1 + chips + has_below + has_above)

    panel_copy.wait()

    def send(way, source, piece):
        start, size = pieces[piece]
        target = (me_c + 2, me_c - 2, z * 2 + other)[way]
        part = gathered.at[source, :, pl.ds(start, size)]
        return pltpu.make_async_remote_copy(
            src_ref=part, dst_ref=part,
            send_sem=panel_send.at[way, source, piece],
            recv_sem=panel_recv.at[source, piece],
            device_id=(me_r, target), device_id_type=MESH,
        )

    def along(source, piece, ways=(0, 1)):
        if 0 in ways:
            @pl.when(z < length - 1)
            def _():
                send(0, source, piece).start()
        if 1 in ways:
            @pl.when(z > 0)
            def _():
                send(1, source, piece).start()

    def arrived(source, piece):
        send(2, source, piece).wait_recv()

    def first_sends():
        send(2, me_c, rest).start()
        for piece in bulk:
            along(me_c, piece)
            send(2, me_c, piece).start()

    def relay_bulk(distance, piece):
        below = (z - distance) * 2 + x
        above = (z + distance) * 2 + x

        @pl.when(z >= distance)
        def _():
            arrived(below, piece)

            @pl.when(z < length - 1)
            def _():
                send(0, below, piece).start()
            send(2, below, piece).start()

        @pl.when(z < length - distance)
        def _():
            arrived(above, piece)

            @pl.when(z > 0)
            def _():
                send(1, above, piece).start()
            send(2, above, piece).start()

    def own_rest():
        along(me_c, rest)
        arrived(z * 2 + other, rest)
        along(z * 2 + other, rest)

    def relay_rest(distance):
        for side in (x, other):
            below = (z - distance) * 2 + side
            above = (z + distance) * 2 + side

            @pl.when(z >= distance)
            def _():
                arrived(below, rest)

                @pl.when(z < length - 1)
                def _():
                    send(0, below, rest).start()

            @pl.when(z < length - distance)
            def _():
                arrived(above, rest)

                @pl.when(z > 0)
                def _():
                    send(1, above, rest).start()

    def each_line(act):
        for at in range(length):
            act(at)

    def last_arrivals():
        for at in range(length):
            for piece in bulk:
                arrived(at * 2 + other, piece)

    def drain():
        for at in range(length):
            for side in (0, 1):
                source = at * 2 + side
                for piece in range(len(pieces)):
                    def up():
                        send(0, source, piece).wait_send()

                    def down():
                        send(1, source, piece).wait_send()

                    use = (piece == rest) | (x == side)
                    pl.when(use & (z < length - 1) & (at <= z))(up)
                    pl.when(use & (z > 0) & (at >= z))(down)
                    if piece == rest:
                        pl.when((x == side) & (at == z))(lambda: send(2, source, piece).wait_send())
                    else:
                        pl.when(x == side)(lambda: send(2, source, piece).wait_send())

    state = {}
    ii = iota((block, block), 0)
    jj = iota((block, block), 1)

    def column(row):
        return jnp.sum(jnp.where(ii == jj, row, 0.0), axis=1, keepdims=True)

    def bookkeeping():
        pivot_row = pivots_ref[...].astype(F32)
        pivot_col = column(pivot_row)
        chosen = jnp.max(jnp.where(pivot_col == jj.astype(F32), 1.0, 0.0), axis=0, keepdims=True)
        free = 1.0 - chosen
        far = jnp.where(pivot_row >= block, 1.0, 0.0)
        which = iota((16, block), 0)
        both = jnp.where(which == 0, free, jnp.where(which == 1, far, 0.0))
        ranks = dot(both.astype(BF16), jnp.where(ii < jj, 1.0, 0.0).astype(BF16))
        far_rank = column(ranks[1:2])
        match = (free > 0.5) & (ranks[0:1] == far_rank)
        source = jnp.sum(jnp.where(match, jj.astype(F32), 0.0), axis=1, keepdims=True)
        state.update(pivot_row=pivot_row, pivot_col=pivot_col, source=source)

    def pick():
        pivot_col, source = state["pivot_col"], state["source"]
        first = (me_r * rows).astype(F32)
        mine = (pivot_col >= first) & (pivot_col < first + rows)
        lead = (me_r == 0).astype(F32)
        index = jnp.where(mine, pivot_col - first, source * lead - (1.0 - lead))
        slab_copy.wait()
        total = jnp.zeros((block, width), F32)
        for start in range(0, rows, block):
            hot = jnp.where((jj + start).astype(F32) == index, 1.0, 0.0).astype(BF16)
            total = total + dot(hot, slab_ref[start:start + block, :])
        picked[...] = total.astype(BF16)

    def core_copy():
        return pltpu.make_async_remote_copy(
            src_ref=picked, dst_ref=picked_in, send_sem=core_sem.at[0], recv_sem=core_sem.at[1],
            device_id=(peer, me_c), device_id_type=MESH,
        )

    def own_homes():
        homes[:, width:] = jnp.ones((block, LANES), BF16)

        @pl.when(me_r == 0)
        def _():
            hot = jnp.where(jj.astype(F32) == state["source"], 1.0, 0.0).astype(BF16)
            homes[:, :width] = dot(hot, slab_ref[:block, :]).astype(BF16)

    half = block // 2

    def chip_copy(step):
        rows_of = pl.ds(pl.multiple_of(core * half, half), half)
        to = ((chip + step) % chips) * 2 + core
        return pltpu.make_async_remote_copy(
            src_ref=merged.at[0, rows_of], dst_ref=merged.at[step, rows_of],
            send_sem=chip_send.at[step], recv_sem=chip_recv.at[step],
            device_id=(to, me_c), device_id_type=MESH,
        )

    def relay_copy(step):
        part = merged.at[step, pl.ds(pl.multiple_of(core * half, half), half)]
        return pltpu.make_async_remote_copy(
            src_ref=part, dst_ref=part, send_sem=relay_send.at[step], recv_sem=relay_recv.at[step],
            device_id=(peer, me_c), device_id_type=MESH,
        )

    def merge():
        core_copy().wait()
        pivot_col = state["pivot_col"]
        lead = (chip == 0).astype(F32)
        second = jnp.where((pivot_col >= rows) & (pivot_col < 2 * rows), lead, 0.0)
        mine, theirs = picked[...].astype(F32), picked_in[...].astype(F32)
        even = (core == 0).astype(F32)
        keep_mine = 1.0 - even * second
        keep_theirs = 1.0 - (1.0 - even) * second
        merged[0] = (mine * keep_mine + theirs * keep_theirs).astype(BF16)
        for step in range(1, chips):
            chip_copy(step).start()

    def relay_chips():
        for step in range(1, chips):
            chip_copy(step).wait()
            relay_copy(step).start()

    def assemble():
        for step in range(1, chips):
            relay_copy(step).wait()
        pivot_col = state["pivot_col"]
        top = jnp.zeros((block, width), F32)
        for step in range(chips):
            low = (((chip + chips - step) % chips) * 2 * rows).astype(F32)
            here = (pivot_col >= low) & (pivot_col < low + 2 * rows)
            top = top + jnp.where(here, merged[step].astype(F32), 0.0)
        state["top"] = top.astype(BF16)

        @pl.when(me_r == 1)
        def _():
            homes[:, :width] = picked_in[...]

        for step in range(1, chips):
            @pl.when((chip > 0) & (chip == step))
            def _():
                homes[:, :width] = merged[step]

    def interchange(start):
        def act():
            row = iota((block, block), 0) + (me_r * rows + start)
            pivot_row = state["pivot_row"]
            hot = jnp.where((row.astype(F32) == pivot_row) & (pivot_row >= block), 1.0, 0.0)
            both = dot(hot.astype(BF16), homes[...])
            taken = both[:, width:] > 0.5
            for lane in range(0, width, LANES):
                kept = slab_ref[start:start + block, lane:lane + LANES].astype(F32)
                new = jnp.where(taken, both[:, lane:lane + LANES], kept)
                pivoted[start:start + block, lane:lane + LANES] = new.astype(BF16)
        return act

    base = min(block, 256)
    small = min(base, 16)
    bi = iota((base, base), 0)
    bj = iota((base, base), 1)
    groups = block // base

    def diagonal(g):
        part = l_top_ref[g * base:(g + 1) * base, g * base:(g + 1) * base].astype(F32)
        return jnp.where(bi > bj, part, 0.0)

    def start_inverse():
        state["x"], state["power"] = [], []
        for g in range(groups):
            near = jnp.where(bi // small == bj // small, diagonal(g), 0.0)
            state["x"].append(jnp.where(bi == bj, 1.0, 0.0) - near)
            state["power"].append(near)

    def power_step():
        for g in range(groups):
            square = dot_high(state["power"][g], state["power"][g])
            state["power"][g] = square
            state["x"][g] = state["x"][g] + dot_high(state["x"][g], square)

    def double(size):
        def act():
            for g in range(groups):
                link = jnp.where(
                    (bi // (2 * size) == bj // (2 * size)) & (bi // size != bj // size), diagonal(g), 0.0
                )
                inv = state["x"][g]
                state["x"][g] = inv - dot_high(inv, dot_high(link, inv))
        return act

    def join():
        for g in range(groups):
            high[g * base:(g + 1) * base, :] = jnp.zeros((base, block), F32)
            high[g * base:(g + 1) * base, g * base:(g + 1) * base] = state["x"][g]

    def join_double(size):
        def act():
            for at in range(0, block, 2 * size):
                a = high[at:at + size, at:at + size]
                b = high[at + size:at + 2 * size, at + size:at + 2 * size]
                c = l_top_ref[at + size:at + 2 * size, at:at + size].astype(F32)
                high[at + size:at + 2 * size, at:at + size] = -dot_high(b, dot_high(c, a))
        return act

    def split():
        whole = high[...]
        top_bits = whole.astype(BF16)
        inverse_hi[...] = top_bits
        inverse_lo[...] = (whole - top_bits.astype(F32)).astype(BF16)

    def solve():
        top = state["top"]
        u_ref[...] = (dot(inverse_hi[...], top) + dot(inverse_lo[...], top)).astype(BF16)

    inverse = [start_inverse]
    size = 2
    while size < small:
        inverse.append(power_step)
        size *= 2
    size = small
    while size < base:
        inverse.append(double(size))
        size *= 2
    inverse.append(join)
    while size < block:
        inverse.append(join_double(size))
        size *= 2
    inverse.append(split)

    first_sends()
    bookkeeping()
    pick()
    core_copy().start()
    own_homes()
    events = [functools.partial(relay_bulk, d, p) for d in range(1, length) for p in bulk]
    events.append(own_rest)
    events += [functools.partial(relay_rest, d) for d in range(1, length)]
    work = [inverse[0], merge] + inverse[1:7] + [relay_chips] + inverse[7:] + [assemble, solve]
    work += [interchange(start) for start in range(0, rows, block)]
    events.append(last_arrivals)
    per = -(-len(work) // max(1, len(events) - 1))
    for event in events[:-1]:
        event()
        for act in work[:per]:
            act()
        work = work[per:]
    for act in work:
        act()
    events[-1]()

    for start in range(0, rows, block):
        panel = gathered[:, :, start:start + block].reshape(block, block).astype(BF16)
        product = lax.dot_general(
            panel, u_ref[...], (((0,), (0,)), ((), ())), preferred_element_type=F32
        )
        out_ref[start:start + block, :] = (pivoted[start:start + block, :].astype(F32) - product).astype(BF16)

    @pl.when(me_r == 0)
    def _():
        out_ref[:block, :] = u_ref[...]

    drain()


def per_device(n_prow, n_pcol, slab, pivots, l_top, l_panel_t):
    rows, width = slab.shape
    block = pivots.shape[0]
    depth = l_panel_t.shape[0]
    kind = BF16 if depth % 16 == 0 else F32
    panel = l_panel_t.astype(kind)
    chips = n_prow // 2
    n_pieces = len(cuts(rows))
    vmem = pl.BlockSpec(memory_space=pltpu.VMEM)
    anywhere = pl.BlockSpec(memory_space=pl.ANY)
    dma = pltpu.SemaphoreType.DMA
    return pl.pallas_call(
        functools.partial(kernel, n_prow, n_pcol),
        out_shape=jax.ShapeDtypeStruct((rows, width), BF16),
        in_specs=[anywhere, vmem, vmem, anywhere],
        out_specs=vmem,
        scratch_shapes=[
            pltpu.VMEM((rows, width), BF16),
            pltpu.VMEM((n_pcol, depth, rows), kind),
            pltpu.VMEM((block, width), BF16),
            pltpu.VMEM((block, width), BF16),
            pltpu.VMEM((chips, block, width), BF16),
            pltpu.VMEM((block, width + LANES), BF16),
            pltpu.VMEM((rows, width), BF16),
            pltpu.VMEM((block, block), BF16),
            pltpu.VMEM((block, block), BF16),
            pltpu.VMEM((block, block), F32),
            pltpu.VMEM((block, width), BF16),
            dma((2,)),
            dma((n_pcol, n_pieces)),
            dma((3, n_pcol, n_pieces)),
            dma((2,)),
            dma((chips,)),
            dma((chips,)),
            dma((chips,)),
            dma((chips,)),
        ],
        compiler_params=pltpu.CompilerParams(collective_id=0, has_side_effects=True),
    )(slab, pivots.reshape(1, block), l_top, panel)


def solution(mesh):
    return jax.shard_map(
        functools.partial(per_device, mesh.shape["prow"], mesh.shape["pcol"]),
        mesh=mesh,
        in_specs=(P("prow", "pcol"), P(), P(), P("pcol", "prow")),
        out_specs=P("prow", "pcol"),
        check_vma=False,
    )
```

```python
import functools

import jax
import jax.numpy as jnp
from jax import lax
from jax.experimental import pallas as pl
from jax.experimental.pallas import tpu as pltpu
from jax.sharding import PartitionSpec as P

MESH = pl.DeviceIdType.MESH
F32 = jnp.float32
BF16 = jnp.bfloat16
LANES = 128


def in_turn(first, second):
    first()
    second()


def dot(a, b):
    return jnp.dot(a, b, preferred_element_type=F32)


def dot_high(a, b):
    return jnp.dot(a, b, preferred_element_type=F32, precision=lax.Precision.HIGHEST)


def iota(shape, axis):
    return lax.broadcasted_iota(jnp.int32, shape, axis)


def cuts(width):
    units = width // LANES
    first = (units * 7) // 16
    second = (units * 14) // 16
    edges = (0, first * LANES, second * LANES, width)
    return [(a, b - a) for a, b in zip(edges[:-1], edges[1:])]


def kernel(
    n_prow, n_pcol,
    slab_hbm, pivots_ref, l_top_hbm, panel_hbm, out_ref,
    slab_ref, l_top_ref, gathered, picked, picked_in, merged, homes, pivoted, inverse_hi, inverse_lo, high, u_ref,
    local_sem, panel_recv, panel_send, core_sem, chip_send, chip_recv, relay_send, relay_recv,
):
    block = l_top_ref.shape[0]
    rows, width = slab_ref.shape
    me_r = lax.axis_index("prow")
    me_c = lax.axis_index("pcol")
    chips = n_prow // 2
    chip, core = me_r // 2, me_r % 2
    peer = me_r + 1 - 2 * core
    length = n_pcol // 2
    z, x = me_c // 2, me_c % 2
    other = 1 - x
    pieces = cuts(gathered.shape[2])
    bulk = range(len(pieces) - 1)
    rest = len(pieces) - 1

    slab_copy = pltpu.make_async_copy(slab_hbm, slab_ref, local_sem.at[0])
    panel_copy = pltpu.make_async_copy(panel_hbm, gathered.at[me_c], local_sem.at[1])
    panel_copy.start()
    slab_copy.start()
    l_top_copy = pltpu.make_async_copy(l_top_hbm, l_top_ref, local_sem.at[2])
    l_top_copy.start()

    barrier = pltpu.get_barrier_semaphore()

    def greet(r, c):
        pl.semaphore_signal(barrier, inc=1, device_id=(r, c), device_id_type=MESH)

    greet(peer, me_c)
    greet(me_r, z * 2 + other)
    for step in range(1, chips):
        greet(((chip + step) % chips) * 2 + core, me_c)

    @pl.when(z > 0)
    def _():
        greet(me_r, me_c - 2)

    @pl.when(z < length - 1)
    def _():
        greet(me_r, me_c + 2)

    has_below = (z + length - 1) // length
    has_above = (2 * length - 2 - z) // length
    pl.semaphore_wait(barrier, 1 + chips + has_below + has_above)

    panel_copy.wait()

    def send(way, source, piece):
        start, size = pieces[piece]
        target = (me_c + 2, me_c - 2, z * 2 + other)[way]
        part = gathered.at[source, :, pl.ds(start, size)]
        return pltpu.make_async_remote_copy(
            src_ref=part, dst_ref=part,
            send_sem=panel_send.at[way, source, piece],
            recv_sem=panel_recv.at[source, piece],
            device_id=(me_r, target), device_id_type=MESH,
        )

    def along(source, piece, ways=(0, 1)):
        if 0 in ways:
            @pl.when(z < length - 1)
            def _():
                send(0, source, piece).start()
        if 1 in ways:
            @pl.when(z > 0)
            def _():
                send(1, source, piece).start()

    def arrived(source, piece):
        send(2, source, piece).wait_recv()

    def first_sends():
        send(2, me_c, rest).start()
        for piece in bulk:
            along(me_c, piece)
            send(2, me_c, piece).start()

    def relay_bulk(distance, piece):
        below = (z - distance) * 2 + x
        above = (z + distance) * 2 + x

        @pl.when(z >= distance)
        def _():
            arrived(below, piece)

            @pl.when(z < length - 1)
            def _():
                send(0, below, piece).start()
            send(2, below, piece).start()

        @pl.when(z < length - distance)
        def _():
            arrived(above, piece)

            @pl.when(z > 0)
            def _():
                send(1, above, piece).start()
            send(2, above, piece).start()

    def own_rest(distance):
        if distance == 0:
            arrived(z * 2 + other, rest)
        for source in (me_c, z * 2 + other):
            @pl.when((z == distance) & (z < length - 1))
            def _():
                send(0, source, rest).start()

            @pl.when((length - 1 - z == distance) & (z > 0))
            def _():
                send(1, source, rest).start()

    def relay_rest(distance):
        for side in (x, other):
            below = (z - distance) * 2 + side
            above = (z + distance) * 2 + side

            @pl.when(z >= distance)
            def _():
                arrived(below, rest)

                @pl.when(z < length - 1)
                def _():
                    send(0, below, rest).start()

            @pl.when(z < length - distance)
            def _():
                arrived(above, rest)

                @pl.when(z > 0)
                def _():
                    send(1, above, rest).start()

    def each_line(act):
        for at in range(length):
            act(at)

    def last_arrivals():
        for at in range(length):
            for piece in bulk:
                arrived(at * 2 + other, piece)

    def drain():
        for at in range(length):
            for side in (0, 1):
                source = at * 2 + side
                for piece in range(len(pieces)):
                    def up():
                        send(0, source, piece).wait_send()

                    def down():
                        send(1, source, piece).wait_send()

                    use = (piece == rest) | (x == side)
                    pl.when(use & (z < length - 1) & (at <= z))(up)
                    pl.when(use & (z > 0) & (at >= z))(down)
                    if piece == rest:
                        pl.when((x == side) & (at == z))(lambda: send(2, source, piece).wait_send())
                    else:
                        pl.when(x == side)(lambda: send(2, source, piece).wait_send())

    state = {}
    ii = iota((block, block), 0)
    jj = iota((block, block), 1)

    def column(row):
        return jnp.sum(jnp.where(ii == jj, row, 0.0), axis=1, keepdims=True)

    def bookkeeping():
        pivot_row = pivots_ref[...].astype(F32)
        pivot_col = column(pivot_row)
        chosen = jnp.max(jnp.where(pivot_col == jj.astype(F32), 1.0, 0.0), axis=0, keepdims=True)
        free = 1.0 - chosen
        far = jnp.where(pivot_row >= block, 1.0, 0.0)
        which = iota((16, block), 0)
        both = jnp.where(which == 0, free, jnp.where(which == 1, far, 0.0))
        ranks = dot(both.astype(BF16), jnp.where(ii < jj, 1.0, 0.0).astype(BF16))
        far_rank = column(ranks[1:2])
        match = (free > 0.5) & (ranks[0:1] == far_rank)
        source = jnp.sum(jnp.where(match, jj.astype(F32), 0.0), axis=1, keepdims=True)
        state.update(pivot_row=pivot_row, pivot_col=pivot_col, source=source)

    def pick():
        pivot_col, source = state["pivot_col"], state["source"]
        first = (me_r * rows).astype(F32)
        mine = (pivot_col >= first) & (pivot_col < first + rows)
        lead = (me_r == 0).astype(F32)
        index = jnp.where(mine, pivot_col - first, source * lead - (1.0 - lead))
        slab_copy.wait()
        total = jnp.zeros((block, width), F32)
        for start in range(0, rows, block):
            hot = jnp.where((jj + start).astype(F32) == index, 1.0, 0.0).astype(BF16)
            total = total + dot(hot, slab_ref[start:start + block, :])
        picked[...] = total.astype(BF16)

    def core_copy():
        return pltpu.make_async_remote_copy(
            src_ref=picked, dst_ref=picked_in, send_sem=core_sem.at[0], recv_sem=core_sem.at[1],
            device_id=(peer, me_c), device_id_type=MESH,
        )

    def own_homes():
        homes[:, width:] = jnp.ones((block, LANES), BF16)

        @pl.when(me_r == 0)
        def _():
            hot = jnp.where(jj.astype(F32) == state["source"], 1.0, 0.0).astype(BF16)
            homes[:, :width] = dot(hot, slab_ref[:block, :]).astype(BF16)

    half = block // 2

    def chip_copy(step):
        rows_of = pl.ds(pl.multiple_of(core * half, half), half)
        to = ((chip + step) % chips) * 2 + core
        return pltpu.make_async_remote_copy(
            src_ref=merged.at[0, rows_of], dst_ref=merged.at[step, rows_of],
            send_sem=chip_send.at[step], recv_sem=chip_recv.at[step],
            device_id=(to, me_c), device_id_type=MESH,
        )

    def relay_copy(step):
        part = merged.at[step, pl.ds(pl.multiple_of(core * half, half), half)]
        return pltpu.make_async_remote_copy(
            src_ref=part, dst_ref=part, send_sem=relay_send.at[step], recv_sem=relay_recv.at[step],
            device_id=(peer, me_c), device_id_type=MESH,
        )

    def merge():
        core_copy().wait()
        pivot_col = state["pivot_col"]
        lead = (chip == 0).astype(F32)
        second = jnp.where((pivot_col >= rows) & (pivot_col < 2 * rows), lead, 0.0)
        mine, theirs = picked[...].astype(F32), picked_in[...].astype(F32)
        even = (core == 0).astype(F32)
        keep_mine = 1.0 - even * second
        keep_theirs = 1.0 - (1.0 - even) * second
        merged[0] = (mine * keep_mine + theirs * keep_theirs).astype(BF16)
        for step in range(1, chips):
            chip_copy(step).start()

    def relay_chips():
        for step in range(1, chips):
            chip_copy(step).wait()
            relay_copy(step).start()

    def assemble():
        for step in range(1, chips):
            relay_copy(step).wait()
        pivot_col = state["pivot_col"]
        top = jnp.zeros((block, width), F32)
        for step in range(chips):
            low = (((chip + chips - step) % chips) * 2 * rows).astype(F32)
            here = (pivot_col >= low) & (pivot_col < low + 2 * rows)
            top = top + jnp.where(here, merged[step].astype(F32), 0.0)
        state["top"] = top.astype(BF16)

        @pl.when(me_r == 1)
        def _():
            homes[:, :width] = picked_in[...]

        for step in range(1, chips):
            @pl.when((chip > 0) & (chip == step))
            def _():
                homes[:, :width] = merged[step]

    def interchange(start):
        def act():
            row = iota((block, block), 0) + (me_r * rows + start)
            pivot_row = state["pivot_row"]
            hot = jnp.where((row.astype(F32) == pivot_row) & (pivot_row >= block), 1.0, 0.0)
            both = dot(hot.astype(BF16), homes[...])
            taken = both[:, width:] > 0.5
            for lane in range(0, width, LANES):
                kept = slab_ref[start:start + block, lane:lane + LANES].astype(F32)
                new = jnp.where(taken, both[:, lane:lane + LANES], kept)
                pivoted[start:start + block, lane:lane + LANES] = new.astype(BF16)
        return act

    base = min(block, 256)
    small = min(base, 16)
    bi = iota((base, base), 0)
    bj = iota((base, base), 1)
    groups = block // base

    def diagonal(g):
        part = l_top_ref[g * base:(g + 1) * base, g * base:(g + 1) * base].astype(F32)
        return jnp.where(bi > bj, part, 0.0)

    def start_inverse():
        l_top_copy.wait()
        state["x"], state["power"] = [], []
        for g in range(groups):
            near = jnp.where(bi // small == bj // small, diagonal(g), 0.0)
            state["x"].append(jnp.where(bi == bj, 1.0, 0.0) - near)
            state["power"].append(near)

    def power_step():
        for g in range(groups):
            square = dot_high(state["power"][g], state["power"][g])
            state["power"][g] = square
            state["x"][g] = state["x"][g] + dot_high(state["x"][g], square)

    def double(size):
        def act():
            for g in range(groups):
                link = jnp.where(
                    (bi // (2 * size) == bj // (2 * size)) & (bi // size != bj // size), diagonal(g), 0.0
                )
                inv = state["x"][g]
                state["x"][g] = inv - dot_high(inv, dot_high(link, inv))
        return act

    def join():
        for g in range(groups):
            high[g * base:(g + 1) * base, :] = jnp.zeros((base, block), F32)
            high[g * base:(g + 1) * base, g * base:(g + 1) * base] = state["x"][g]

    def join_double(size):
        def act():
            for at in range(0, block, 2 * size):
                a = high[at:at + size, at:at + size]
                b = high[at + size:at + 2 * size, at + size:at + 2 * size]
                c = l_top_ref[at + size:at + 2 * size, at:at + size].astype(F32)
                high[at + size:at + 2 * size, at:at + size] = -dot_high(b, dot_high(c, a))
        return act

    def split():
        whole = high[...]
        top_bits = whole.astype(BF16)
        inverse_hi[...] = top_bits
        inverse_lo[...] = (whole - top_bits.astype(F32)).astype(BF16)

    def solve():
        top = state["top"]
        u_ref[...] = (dot(inverse_hi[...], top) + dot(inverse_lo[...], top)).astype(BF16)

    inverse = [start_inverse]
    size = 2
    while size < small:
        inverse.append(power_step)
        size *= 2
    size = small
    while size < base:
        inverse.append(double(size))
        size *= 2
    inverse.append(join)
    while size < block:
        inverse.append(join_double(size))
        size *= 2
    inverse.append(split)

    first_sends()
    bookkeeping()
    pick()
    core_copy().start()
    own_homes()
    events = [functools.partial(own_rest, 0)]
    for distance in range(1, length):
        events += [functools.partial(relay_bulk, distance, piece) for piece in bulk]
        events[-1] = functools.partial(in_turn, events[-1], functools.partial(own_rest, distance))
    events += [functools.partial(relay_rest, distance) for distance in range(1, length)]
    work = [inverse[0], merge] + inverse[1:7] + [relay_chips] + inverse[7:] + [assemble, solve]
    work += [interchange(start) for start in range(0, rows, block)]
    events.append(last_arrivals)
    per = -(-len(work) // max(1, len(events) - 1))
    for event in events[:-1]:
        event()
        for act in work[:per]:
            act()
        work = work[per:]
    for act in work:
        act()
    events[-1]()

    for start in range(0, rows, block):
        panel = gathered[:, :, start:start + block].reshape(block, block).astype(BF16)
        product = lax.dot_general(
            panel, u_ref[...], (((0,), (0,)), ((), ())), preferred_element_type=F32
        )
        out_ref[start:start + block, :] = (pivoted[start:start + block, :].astype(F32) - product).astype(BF16)

    @pl.when(me_r == 0)
    def _():
        out_ref[:block, :] = u_ref[...]

    drain()


def per_device(n_prow, n_pcol, slab, pivots, l_top, l_panel_t):
    rows, width = slab.shape
    block = pivots.shape[0]
    depth = l_panel_t.shape[0]
    kind = BF16 if depth % 16 == 0 else F32
    panel = l_panel_t.astype(kind)
    chips = n_prow // 2
    n_pieces = len(cuts(rows))
    vmem = pl.BlockSpec(memory_space=pltpu.VMEM)
    anywhere = pl.BlockSpec(memory_space=pltpu.HBM)
    dma = pltpu.SemaphoreType.DMA
    return pl.pallas_call(
        functools.partial(kernel, n_prow, n_pcol),
        out_shape=pltpu.VMEM((rows, width), BF16),
        in_specs=[anywhere, vmem, anywhere, anywhere],
        out_specs=vmem,
        scratch_shapes=[
            pltpu.VMEM((rows, width), BF16),
            pltpu.VMEM((block, block), BF16),
            pltpu.VMEM((n_pcol, depth, rows), kind),
            pltpu.VMEM((block, width), BF16),
            pltpu.VMEM((block, width), BF16),
            pltpu.VMEM((chips, block, width), BF16),
            pltpu.VMEM((block, width + LANES), BF16),
            pltpu.VMEM((rows, width), BF16),
            pltpu.VMEM((block, block), BF16),
            pltpu.VMEM((block, block), BF16),
            pltpu.VMEM((block, block), F32),
            pltpu.VMEM((block, width), BF16),
            dma((3,)),
            dma((n_pcol, n_pieces)),
            dma((3, n_pcol, n_pieces)),
            dma((2,)),
            dma((chips,)),
            dma((chips,)),
            dma((chips,)),
            dma((chips,)),
        ],
        compiler_params=pltpu.CompilerParams(collective_id=0, has_side_effects=True, vmem_limit_bytes=60 * 2**20),
    )(slab, pivots.reshape(1, block), l_top, panel)


def solution(mesh):
    return jax.shard_map(
        functools.partial(per_device, mesh.shape["prow"], mesh.shape["pcol"]),
        mesh=mesh,
        in_specs=(P("prow", "pcol"), P(), P(), P("pcol", "prow")),
        out_specs=P("prow", "pcol"),
        check_vma=False,
    )
```

```python
import functools

import jax
import jax.numpy as jnp
from jax import lax
from jax.experimental import pallas as pl
from jax.experimental.pallas import tpu as pltpu
from jax.sharding import PartitionSpec as P

MESH = pl.DeviceIdType.MESH
F32 = jnp.float32
BF16 = jnp.bfloat16
LANES = 128


def in_turn(first, second):
    first()
    second()


def dot(a, b):
    return jnp.dot(a, b, preferred_element_type=F32)


def dot_high(a, b):
    return jnp.dot(a, b, preferred_element_type=F32, precision=lax.Precision.HIGHEST)


def iota(shape, axis):
    return lax.broadcasted_iota(jnp.int32, shape, axis)


def cuts(width):
    units = width // LANES
    edges = [(units * part) // 16 * LANES for part in (0, 6, 15, 16)]
    return [(a, b - a) for a, b in zip(edges[:-1], edges[1:])]


def kernel(
    n_prow, n_pcol,
    slab_hbm, pivots_ref, l_top_hbm, panel_hbm, out_ref,
    slab_ref, l_top_ref, gathered, picked, picked_in, merged, homes, pivoted, inverse_hi, inverse_lo, high, u_ref,
    local_sem, panel_recv, panel_send, core_sem, chip_send, chip_recv, relay_send, relay_recv,
):
    block = l_top_ref.shape[0]
    rows, width = slab_ref.shape
    me_r = lax.axis_index("prow")
    me_c = lax.axis_index("pcol")
    chips = n_prow // 2
    chip, core = me_r // 2, me_r % 2
    peer = me_r + 1 - 2 * core
    length = n_pcol // 2
    z, x = me_c // 2, me_c % 2
    other = 1 - x
    pieces = cuts(gathered.shape[2])
    bulk = range(len(pieces) - 1)
    rest = len(pieces) - 1

    slab_copy = pltpu.make_async_copy(slab_hbm, slab_ref, local_sem.at[0])
    panel_copy = pltpu.make_async_copy(panel_hbm, gathered.at[me_c], local_sem.at[1])
    panel_copy.start()
    slab_copy.start()
    l_top_copy = pltpu.make_async_copy(l_top_hbm, l_top_ref, local_sem.at[2])
    l_top_copy.start()

    barrier = pltpu.get_barrier_semaphore()

    def greet(r, c):
        pl.semaphore_signal(barrier, inc=1, device_id=(r, c), device_id_type=MESH)

    greet(peer, me_c)
    greet(me_r, z * 2 + other)
    for step in range(1, chips):
        greet(((chip + step) % chips) * 2 + core, me_c)

    @pl.when(z > 0)
    def _():
        greet(me_r, me_c - 2)

    @pl.when(z < length - 1)
    def _():
        greet(me_r, me_c + 2)

    has_below = (z + length - 1) // length
    has_above = (2 * length - 2 - z) // length
    pl.semaphore_wait(barrier, 1 + chips + has_below + has_above)

    panel_copy.wait()

    def send(way, source, piece):
        start, size = pieces[piece]
        target = (me_c + 2, me_c - 2, z * 2 + other)[way]
        part = gathered.at[source, :, pl.ds(start, size)]
        return pltpu.make_async_remote_copy(
            src_ref=part, dst_ref=part,
            send_sem=panel_send.at[way, source, piece],
            recv_sem=panel_recv.at[source, piece],
            device_id=(me_r, target), device_id_type=MESH,
        )

    def along(source, piece, ways=(0, 1)):
        if 0 in ways:
            @pl.when(z < length - 1)
            def _():
                send(0, source, piece).start()
        if 1 in ways:
            @pl.when(z > 0)
            def _():
                send(1, source, piece).start()

    def arrived(source, piece):
        send(2, source, piece).wait_recv()

    def first_sends():
        send(2, me_c, rest).start()
        for piece in bulk:
            along(me_c, piece)
            send(2, me_c, piece).start()

    def relay_bulk(distance, piece):
        below = (z - distance) * 2 + x
        above = (z + distance) * 2 + x

        @pl.when(z >= distance)
        def _():
            arrived(below, piece)

            @pl.when(z < length - 1)
            def _():
                send(0, below, piece).start()
            send(2, below, piece).start()

        @pl.when(z < length - distance)
        def _():
            arrived(above, piece)

            @pl.when(z > 0)
            def _():
                send(1, above, piece).start()
            send(2, above, piece).start()

    def own_rest(distance):
        if distance == 0:
            arrived(z * 2 + other, rest)
        for source in (me_c, z * 2 + other):
            @pl.when((z == distance) & (z < length - 1))
            def _():
                send(0, source, rest).start()

            @pl.when((length - 1 - z == distance) & (z > 0))
            def _():
                send(1, source, rest).start()

    def relay_rest(distance):
        for side in (x, other):
            below = (z - distance) * 2 + side
            above = (z + distance) * 2 + side

            @pl.when(z >= distance)
            def _():
                arrived(below, rest)

                @pl.when(z < length - 1)
                def _():
                    send(0, below, rest).start()

            @pl.when(z < length - distance)
            def _():
                arrived(above, rest)

                @pl.when(z > 0)
                def _():
                    send(1, above, rest).start()

    def each_line(act):
        for at in range(length):
            act(at)

    def last_arrivals():
        for at in range(length):
            for piece in bulk:
                arrived(at * 2 + other, piece)

    def drain():
        for at in range(length):
            for side in (0, 1):
                source = at * 2 + side
                for piece in range(len(pieces)):
                    def up():
                        send(0, source, piece).wait_send()

                    def down():
                        send(1, source, piece).wait_send()

                    use = (piece == rest) | (x == side)
                    pl.when(use & (z < length - 1) & (at <= z))(up)
                    pl.when(use & (z > 0) & (at >= z))(down)
                    if piece == rest:
                        pl.when((x == side) & (at == z))(lambda: send(2, source, piece).wait_send())
                    else:
                        pl.when(x == side)(lambda: send(2, source, piece).wait_send())

    state = {}
    ii = iota((block, block), 0)
    jj = iota((block, block), 1)

    def column(row):
        return jnp.sum(jnp.where(ii == jj, row, 0.0), axis=1, keepdims=True)

    def bookkeeping():
        pivot_row = pivots_ref[...].astype(F32)
        pivot_col = column(pivot_row)
        chosen = jnp.max(jnp.where(pivot_col == jj.astype(F32), 1.0, 0.0), axis=0, keepdims=True)
        free = 1.0 - chosen
        far = jnp.where(pivot_row >= block, 1.0, 0.0)
        which = iota((16, block), 0)
        both = jnp.where(which == 0, free, jnp.where(which == 1, far, 0.0))
        ranks = dot(both.astype(BF16), jnp.where(ii < jj, 1.0, 0.0).astype(BF16))
        far_rank = column(ranks[1:2])
        match = (free > 0.5) & (ranks[0:1] == far_rank)
        source = jnp.sum(jnp.where(match, jj.astype(F32), 0.0), axis=1, keepdims=True)
        state.update(pivot_row=pivot_row, pivot_col=pivot_col, source=source)

    def pick():
        pivot_col, source = state["pivot_col"], state["source"]
        first = (me_r * rows).astype(F32)
        mine = (pivot_col >= first) & (pivot_col < first + rows)
        lead = (me_r == 0).astype(F32)
        index = jnp.where(mine, pivot_col - first, source * lead - (1.0 - lead))
        slab_copy.wait()
        total = jnp.zeros((block, width), F32)
        for start in range(0, rows, block):
            hot = jnp.where((jj + start).astype(F32) == index, 1.0, 0.0).astype(BF16)
            total = total + dot(hot, slab_ref[start:start + block, :])
        picked[...] = total.astype(BF16)

    def core_copy():
        return pltpu.make_async_remote_copy(
            src_ref=picked, dst_ref=picked_in, send_sem=core_sem.at[0], recv_sem=core_sem.at[1],
            device_id=(peer, me_c), device_id_type=MESH,
        )

    def own_homes():
        homes[:, width:] = jnp.ones((block, LANES), BF16)

        @pl.when(me_r == 0)
        def _():
            hot = jnp.where(jj.astype(F32) == state["source"], 1.0, 0.0).astype(BF16)
            homes[:, :width] = dot(hot, slab_ref[:block, :]).astype(BF16)

    half = block // 2

    def chip_copy(step):
        rows_of = pl.ds(pl.multiple_of(core * half, half), half)
        to = ((chip + step) % chips) * 2 + core
        return pltpu.make_async_remote_copy(
            src_ref=merged.at[0, rows_of], dst_ref=merged.at[step, rows_of],
            send_sem=chip_send.at[step], recv_sem=chip_recv.at[step],
            device_id=(to, me_c), device_id_type=MESH,
        )

    def relay_copy(step):
        part = merged.at[step, pl.ds(pl.multiple_of(core * half, half), half)]
        return pltpu.make_async_remote_copy(
            src_ref=part, dst_ref=part, send_sem=relay_send.at[step], recv_sem=relay_recv.at[step],
            device_id=(peer, me_c), device_id_type=MESH,
        )

    def merge():
        core_copy().wait()
        pivot_col = state["pivot_col"]
        lead = (chip == 0).astype(F32)
        second = jnp.where((pivot_col >= rows) & (pivot_col < 2 * rows), lead, 0.0)
        mine, theirs = picked[...].astype(F32), picked_in[...].astype(F32)
        even = (core == 0).astype(F32)
        keep_mine = 1.0 - even * second
        keep_theirs = 1.0 - (1.0 - even) * second
        merged[0] = (mine * keep_mine + theirs * keep_theirs).astype(BF16)
        for step in range(1, chips):
            chip_copy(step).start()

    def relay_chips():
        for step in range(1, chips):
            chip_copy(step).wait()
            relay_copy(step).start()

    def assemble():
        for step in range(1, chips):
            relay_copy(step).wait()
        pivot_col = state["pivot_col"]
        top = jnp.zeros((block, width), F32)
        for step in range(chips):
            low = (((chip + chips - step) % chips) * 2 * rows).astype(F32)
            here = (pivot_col >= low) & (pivot_col < low + 2 * rows)
            top = top + jnp.where(here, merged[step].astype(F32), 0.0)
        state["top"] = top.astype(BF16)

        @pl.when(me_r == 1)
        def _():
            homes[:, :width] = picked_in[...]

        for step in range(1, chips):
            @pl.when((chip > 0) & (chip == step))
            def _():
                homes[:, :width] = merged[step]

    def interchange(start):
        def act():
            row = iota((block, block), 0) + (me_r * rows + start)
            pivot_row = state["pivot_row"]
            hot = jnp.where((row.astype(F32) == pivot_row) & (pivot_row >= block), 1.0, 0.0)
            both = dot(hot.astype(BF16), homes[...])
            taken = both[:, width:] > 0.5
            for lane in range(0, width, LANES):
                kept = slab_ref[start:start + block, lane:lane + LANES].astype(F32)
                new = jnp.where(taken, both[:, lane:lane + LANES], kept)
                pivoted[start:start + block, lane:lane + LANES] = new.astype(BF16)
        return act

    base = min(block, 256)
    small = min(base, 16)
    bi = iota((base, base), 0)
    bj = iota((base, base), 1)
    groups = block // base

    def diagonal(g):
        part = l_top_ref[g * base:(g + 1) * base, g * base:(g + 1) * base].astype(F32)
        return jnp.where(bi > bj, part, 0.0)

    def start_inverse():
        l_top_copy.wait()
        state["x"], state["power"] = [], []
        for g in range(groups):
            near = jnp.where(bi // small == bj // small, diagonal(g), 0.0)
            state["x"].append(jnp.where(bi == bj, 1.0, 0.0) - near)
            state["power"].append(near)

    def power_step():
        for g in range(groups):
            square = dot_high(state["power"][g], state["power"][g])
            state["power"][g] = square
            state["x"][g] = state["x"][g] + dot_high(state["x"][g], square)

    def double(size):
        def act():
            for g in range(groups):
                link = jnp.where(
                    (bi // (2 * size) == bj // (2 * size)) & (bi // size != bj // size), diagonal(g), 0.0
                )
                inv = state["x"][g]
                state["x"][g] = inv - dot_high(inv, dot_high(link, inv))
        return act

    def join():
        for g in range(groups):
            high[g * base:(g + 1) * base, :] = jnp.zeros((base, block), F32)
            high[g * base:(g + 1) * base, g * base:(g + 1) * base] = state["x"][g]

    def join_double(size):
        def act():
            for at in range(0, block, 2 * size):
                a = high[at:at + size, at:at + size]
                b = high[at + size:at + 2 * size, at + size:at + 2 * size]
                c = l_top_ref[at + size:at + 2 * size, at:at + size].astype(F32)
                high[at + size:at + 2 * size, at:at + size] = -dot_high(b, dot_high(c, a))
        return act

    def split():
        whole = high[...]
        top_bits = whole.astype(BF16)
        inverse_hi[...] = top_bits
        inverse_lo[...] = (whole - top_bits.astype(F32)).astype(BF16)

    def solve():
        top = state["top"]
        u_ref[...] = (dot(inverse_hi[...], top) + dot(inverse_lo[...], top)).astype(BF16)

    inverse = [start_inverse]
    size = 2
    while size < small:
        inverse.append(power_step)
        size *= 2
    size = small
    while size < base:
        inverse.append(double(size))
        size *= 2
    inverse.append(join)
    while size < block:
        inverse.append(join_double(size))
        size *= 2
    inverse.append(split)

    first_sends()
    bookkeeping()
    pick()
    core_copy().start()
    own_homes()
    events = [functools.partial(own_rest, 0)]
    for distance in range(1, length):
        events += [functools.partial(relay_bulk, distance, piece) for piece in bulk]
        events[-1] = functools.partial(in_turn, events[-1], functools.partial(own_rest, distance))
    events += [functools.partial(relay_rest, distance) for distance in range(1, length)]
    work = [inverse[0], merge] + inverse[1:7] + [relay_chips] + inverse[7:] + [assemble, solve]
    work += [interchange(start) for start in range(0, rows, block)]
    events.append(last_arrivals)
    per = -(-len(work) // max(1, len(events) - 1))
    for event in events[:-1]:
        event()
        for act in work[:per]:
            act()
        work = work[per:]
    for act in work:
        act()
    events[-1]()

    for start in range(0, rows, block):
        panel = gathered[:, :, start:start + block].reshape(block, block).astype(BF16)
        product = lax.dot_general(
            panel, u_ref[...], (((0,), (0,)), ((), ())), preferred_element_type=F32
        )
        out_ref[start:start + block, :] = (pivoted[start:start + block, :].astype(F32) - product).astype(BF16)

    @pl.when(me_r == 0)
    def _():
        out_ref[:block, :] = u_ref[...]

    drain()


def per_device(n_prow, n_pcol, slab, pivots, l_top, l_panel_t):
    rows, width = slab.shape
    block = pivots.shape[0]
    depth = l_panel_t.shape[0]
    kind = BF16 if depth % 16 == 0 else F32
    panel = l_panel_t.astype(kind)
    chips = n_prow // 2
    n_pieces = len(cuts(rows))
    vmem = pl.BlockSpec(memory_space=pltpu.VMEM)
    anywhere = pl.BlockSpec(memory_space=pltpu.HBM)
    dma = pltpu.SemaphoreType.DMA
    return pl.pallas_call(
        functools.partial(kernel, n_prow, n_pcol),
        out_shape=pltpu.VMEM((rows, width), BF16),
        in_specs=[anywhere, vmem, anywhere, anywhere],
        out_specs=vmem,
        scratch_shapes=[
            pltpu.VMEM((rows, width), BF16),
            pltpu.VMEM((block, block), BF16),
            pltpu.VMEM((n_pcol, depth, rows), kind),
            pltpu.VMEM((block, width), BF16),
            pltpu.VMEM((block, width), BF16),
            pltpu.VMEM((chips, block, width), BF16),
            pltpu.VMEM((block, width + LANES), BF16),
            pltpu.VMEM((rows, width), BF16),
            pltpu.VMEM((block, block), BF16),
            pltpu.VMEM((block, block), BF16),
            pltpu.VMEM((block, block), F32),
            pltpu.VMEM((block, width), BF16),
            dma((3,)),
            dma((n_pcol, n_pieces)),
            dma((3, n_pcol, n_pieces)),
            dma((2,)),
            dma((chips,)),
            dma((chips,)),
            dma((chips,)),
            dma((chips,)),
        ],
        compiler_params=pltpu.CompilerParams(collective_id=0, has_side_effects=True, vmem_limit_bytes=60 * 2**20),
    )(slab, pivots.reshape(1, block), l_top, panel)


def solution(mesh):
    return jax.shard_map(
        functools.partial(per_device, mesh.shape["prow"], mesh.shape["pcol"]),
        mesh=mesh,
        in_specs=(P("prow", "pcol"), P(), P(), P("pcol", "prow")),
        out_specs=P("prow", "pcol"),
        check_vma=False,
    )
```
